512 devices in a mesh: dom: 64 (over x, y, core), mem: 8 (over z).
Axes of the slice: x: 4, y: 8, z: 8, core: 2. Of those that a mesh axis runs over, the one named last changes fastest.
Arguments:
- ensemble: bfloat16 [48, 32, 262144], P('mem', None, 'dom'), may hold values from -6 to 6
- observed: float32 [32, 65536], P(None, 'dom'), may hold values from -6 to 6
- tile_weight: bfloat16 [6144, 128, 128], P('dom')
- tile_block: int32 [6144], P('dom'), may hold values from 0 to 31
- tile_target: int32 [6144], P('dom'), may hold values from 0 to 511, as said below
- tile_count: int32 [64], P('dom'), may hold values from 48 to 96, as said below
Outputs:
- crps: float32 [32, 65536], P(None, 'dom')
The draws below stay inside these ranges and needn't reach their ends.
Inputs may be any that keep to these rules, and one draw needn't show every extreme that they name: `tile_block`: a slot's source block, counted within its partition's cells. `tile_target`: slot k belongs to partition p = k // 96; its target tile is owned by one of the partitions p - 4 to p + 4, where partition o owns the 8 target tiles from o * 8 on. The live slots of partition p are the first tile_count[p] of its list; the rest are padding.
All inputs are finite; a program needn't handle non-finite values.
Results may differ from the reference program's by a relative error of at most 0.0003.
Values sent between devices are 32-bit elements; how exact they have to be, the bound alone decides.
No kernel may reach another device: no remote copies, remote signals or barrier semaphores. Data moves between devices by JAX's collectives and lax.ppermute only.
A program may use at most 64 MiB of HBM per device.

```python
import math
import jax
import jax.numpy as jnp
from jax import lax

BLOCK = 128
REACH = 4
LEV = 32
SRC_DEV = 4096
TGT_DEV = 1024
TILES_DEV = 96
PARTITIONS = 64
MEMBERS = 48
SRC = 262144
TGT = 65536
TILES = 6144


def draw_tile_weight(key, part):
    key_diag, key_off = jax.random.split(key, 2)
    shape = (TILES, BLOCK, BLOCK)
    unit_diag = jnp.eye(BLOCK, dtype=jnp.float32)
    overall = (0.75 * TILES_DEV * BLOCK / TGT_DEV) ** (-0.5)
    diagonal = jax.random.uniform(key_diag, (TILES, 1, BLOCK), jnp.float32, 0.4, 1.2)
    rough = 0.03 * jax.random.normal(key_off, shape, jnp.float32)
    weights = (rough * (1.0 - unit_diag) + diagonal * unit_diag) * overall
    return weights.astype(jnp.bfloat16)


def draw_tile_target(key, part):
    partition = jnp.arange(TILES, dtype=jnp.int32) // TILES_DEV
    slot_place = jnp.arange(TILES, dtype=jnp.int32) % TILES_DEV
    lowest = jnp.maximum(partition - REACH, 0)
    highest = jnp.minimum(partition + REACH, PARTITIONS - 1)
    key_owner, key_tile = jax.random.split(key)
    owner = jax.random.randint(key_owner, (TILES,), lowest, highest + 1)
    owner = jnp.where(slot_place == 0, highest, owner)
    owner = jnp.where(slot_place == 1, lowest, owner)
    owned = TGT_DEV // BLOCK
    inner = jax.random.randint(key_tile, (TILES,), 0, owned)
    return (owner * owned + inner).astype(jnp.int32)


def draw_tile_count(key, part):
    key_count, key_full = jax.random.split(key)
    counts = jax.random.randint(key_count, (PARTITIONS,), TILES_DEV // 2, TILES_DEV + 1)
    fullest = jax.random.randint(key_full, (), 0, PARTITIONS)
    return jnp.where(jnp.arange(PARTITIONS, dtype=jnp.int32) == fullest, TILES_DEV, counts).astype(jnp.int32)


def set_ends(result, own_key, smallest, largest):
    longest = result.shape.index(max(result.shape))
    spots = []
    for shift in (0, 1):
        where = [jax.random.randint(jax.random.fold_in(own_key, axis), (), 0, length) for axis, length in enumerate(result.shape)]
        where[longest] = (where[longest] + shift) % result.shape[longest]
        spots.append(tuple(where))
    return result.at[spots[0]].set(smallest).at[spots[1]].set(largest)


def steps_of(own_key, shape, cuts, low, top_value):
    level = 1.0
    for axis_at, blocks in cuts:
        heights = jax.random.uniform(jax.random.fold_in(jax.random.fold_in(own_key, 6), axis_at), (blocks,), jnp.float32, low / len(cuts), top_value / len(cuts))
        level = level * jnp.repeat(jnp.exp(heights), shape[axis_at] // blocks).reshape((-1,) + (1,) * (len(shape) - 1 - axis_at))
    return level


def centred(own_key, dims, scale, limit, cuts=(), held_as=jnp.bfloat16):
    array = scale * jax.random.normal(own_key, dims, jnp.float32)
    if cuts:
        array = array * steps_of(own_key, dims, cuts, -0.22, 0.18)
    return jnp.clip(array, -limit, limit).astype(held_as)


def setup_inputs(seed: int = 0) -> dict:
    splits = jax.random.split(jax.random.key(seed), 7)
    ensemble = centred(splits[0], (MEMBERS, LEV, SRC), 1.0, 6.0, ((0, 8), (2, 64)))
    observed = centred(splits[1], (LEV, TGT), 1.0, 6.0, ((1, 64),), jnp.float32)
    tile_weight = draw_tile_weight(jax.random.fold_in(splits[6], 71), 0)
    tile_block = set_ends(jax.random.randint(splits[3], (TILES,), 0, SRC_DEV // BLOCK), jax.random.fold_in(splits[3], 1), 0, (SRC_DEV // BLOCK) - 1).astype(jnp.int32)
    tile_target = draw_tile_target(jax.random.fold_in(splits[6], 71), 0)
    tile_count = draw_tile_count(jax.random.fold_in(splits[6], 71), 0)
    return dict(ensemble=ensemble, observed=observed, tile_weight=tile_weight, tile_block=tile_block, tile_target=tile_target, tile_count=tile_count)


def pair_total(left_set, right_set, widest):
    flat_left = left_set.reshape(left_set.shape[0], -1)
    flat_right = right_set.reshape(right_set.shape[0], -1)
    total_columns = flat_left.shape[1]
    block_span = math.gcd(total_columns, widest)

    def block_pairs(first_column):
        left_cols = lax.dynamic_slice_in_dim(flat_left, first_column, block_span, 1)
        right_cols = lax.dynamic_slice_in_dim(flat_right, first_column, block_span, 1)
        return jnp.sum(jnp.abs(left_cols[:, None, :] - right_cols[None, :, :]), axis=(0, 1))

    column_starts = jnp.arange(total_columns // block_span, dtype=jnp.int32) * block_span
    return lax.map(block_pairs, column_starts).reshape(left_set.shape[1:])


def reference(ensemble, observed, tile_weight, tile_block, tile_target, tile_count):
    members = ensemble.shape[0]
    channels = members * LEV
    block_count = SRC_DEV // BLOCK
    values = ensemble.reshape(channels, PARTITIONS, block_count, BLOCK)
    values = jnp.moveaxis(values, 1, 0)
    weights = tile_weight.reshape(PARTITIONS, TILES_DEV, BLOCK, BLOCK)
    blocks = tile_block.reshape(PARTITIONS, TILES_DEV)
    targets = tile_target.reshape(PARTITIONS, TILES_DEV)
    slot_index = jnp.arange(TILES_DEV, dtype=jnp.int32)

    def add_partition(summed, inputs):
        part_values, part_weights, part_blocks, part_targets, part_count = inputs
        picked = jnp.take(part_values, part_blocks.astype(jnp.int32), axis=1).astype(jnp.float32)
        partial_value = jnp.einsum('csi,sij->scj', picked, part_weights.astype(jnp.float32), precision=lax.Precision.HIGHEST)
        is_live = (slot_index < part_count).astype(jnp.float32)
        partial_value = partial_value * is_live[:, None, None]
        return summed.at[part_targets.astype(jnp.int32)].add(partial_value), None

    initial = jnp.zeros((PARTITIONS * TGT_DEV // BLOCK, channels, BLOCK), jnp.float32)
    summed, ignored = lax.scan(add_partition, initial, (values, weights, blocks, targets, tile_count))
    tile_total = PARTITIONS * TGT_DEV // BLOCK
    remapped = summed.reshape(tile_total, members, LEV, BLOCK).transpose(1, 2, 0, 3).reshape(members, LEV, tile_total * BLOCK)
    skill_sum = jnp.sum(jnp.abs(remapped - observed[None]), axis=0)
    spread = pair_total(remapped, remapped, 16384)
    return skill_sum / members - spread / (2.0 * members * (members - 1))
```

```python
import functools

import jax
import jax.numpy as jnp
from jax import lax
from jax.experimental import pallas as pl
from jax.experimental.pallas import tpu as pltpu
from jax.sharding import PartitionSpec as P

CHUNKS = (16, 16)

FAR = {4: 0, -3: 1, -4: 2}
NEAR = {2: 0, 3: 1, 0: 2, -1: 3, -2: 4, 1: 5}
UNROLL = 4


def coded(table):
    return sum(table.get(u, 7) << (3 * (u + 4)) for u in range(-4, 5))


def remap_kernel(codes, parts, split, chunks, block_ref, target_ref, count_ref, ens_ref, weight_ref, *rest):
    outs, (acc, weights, slots, sems) = rest[:-4], rest[-4:]
    groups, levels, _ = ens_ref.shape
    total = target_ref.shape[0]
    owned = 8
    pieces = sems.shape[0]
    span = total // pieces
    copies = [
        pltpu.make_async_copy(
            weight_ref.at[pl.ds(piece * span, span)], weights.at[pl.ds(piece * span, span)], sems.at[piece]
        )
        for piece in range(pieces)
    ]
    for copy in copies:
        copy.start()
    device = lax.axis_index("dom")
    side = 1 - 2 * lax.rem(device, 2)
    live = count_ref[0]
    dump = parts * owned

    def listed(slot, found):
        target = target_ref[slot]
        u = side * ((target >> 3) - device)
        code = (codes >> (3 * (u + 4))) & 7
        slots[found] = slot * 256 + code * owned + (target & 7)
        return found + jnp.where((code < 7) & (slot < live), 1, 0)

    found = lax.fori_loop(0, total, listed, jnp.int32(0), unroll=8)
    for extra in range(UNROLL):
        slots[found + extra] = dump

    def cleared(tile, carry):
        acc[tile] = jnp.zeros(acc.shape[1:], jnp.float32)
        return carry

    lax.fori_loop(0, dump, cleared, 0)
    for copy in copies:
        copy.wait()

    def added(step, carry):
        results = []
        for offset in range(UNROLL):
            entry = slots[step * UNROLL + offset]
            slot = entry >> 8
            first = pl.multiple_of(block_ref[slot] * 128, 128)
            picked = ens_ref[:, :, pl.ds(first, 128)].reshape(groups * levels, 128)
            results.append(
                (entry & 255, jnp.dot(picked, weights[slot], preferred_element_type=jnp.float32))
            )
        for tile, result in results:
            acc[tile] += result
        return carry

    lax.fori_loop(0, (found + UNROLL - 1) // UNROLL, added, 0)

    def stored(tile, carry):
        start = 0
        for index, length in enumerate(chunks):
            for low, high, out in ((0, split, outs[2 * index]), (split, parts, outs[2 * index + 1])):
                for part in range(low, high):
                    for group in range(groups):
                        out[part - low, tile, group] = acc[part * owned + tile, pl.ds(group * levels + start, length)]
            start += length
        return carry

    lax.fori_loop(0, owned, stored, 0)


def remap(table, parts, split, chunks, ensemble, tile_weight, tile_block, tile_target, tile_count):
    groups, levels, _ = ensemble.shape
    slots = tile_block.shape[0]
    shapes = []
    for length in chunks:
        for count in (split, parts - split):
            shapes.append(jax.ShapeDtypeStruct((count, 8, groups, length, 128), jnp.float32))
    smem = pl.BlockSpec(memory_space=pltpu.SMEM)
    vmem = pl.BlockSpec(memory_space=pltpu.VMEM)
    outs = pl.pallas_call(
        functools.partial(remap_kernel, coded(table), parts, split, chunks),
        out_shape=shapes,
        in_specs=[smem, smem, smem, vmem, pl.BlockSpec(memory_space=pl.ANY)],
        out_specs=[vmem] * len(shapes),
        scratch_shapes=[
            pltpu.VMEM((parts * 8 + 1, groups * levels, 128), jnp.float32),
            pltpu.VMEM(tile_weight.shape, tile_weight.dtype),
            pltpu.SMEM((slots + UNROLL,), jnp.int32),
            pltpu.SemaphoreType.DMA((4,)),
        ],
        cost_estimate=pl.CostEstimate(
            flops=2 * slots * groups * levels * 128 * 128, bytes_accessed=12_000_000, transcendentals=0
        ),
        compiler_params=pltpu.CompilerParams(vmem_limit_bytes=20 * 1024 * 1024),
    )(tile_block, tile_target, tile_count, ensemble, tile_weight)
    return [outs[2 * index : 2 * index + 2] for index in range(len(chunks))]


def score_kernel(first, copies, members_ref, observed_ref, *rest):
    before, out = rest[:-1], rest[-1]
    members, length, cells = members_ref.shape
    column = pl.multiple_of(lax.axis_index("mem") * cells, cells)
    done = 0
    scores = []
    for ref in before:
        scores.append((done, ref[...]))
        done += ref.shape[0]
    for low in range(0, length, 8):
        observed = observed_ref[pl.ds(first + low, 8), pl.ds(column, cells)]
        skill = jnp.zeros((8, cells), jnp.float32)
        spread = jnp.zeros((8, cells), jnp.float32)
        values = [members_ref[member, pl.ds(low, 8)] for member in range(members)]
        for left in range(members):
            skill = skill + jnp.abs(values[left] - observed)
            row = None
            for right in range(left + 1, members):
                gap = jnp.abs(values[left] - values[right])
                row = gap if row is None else row + gap
            if row is not None:
                spread = spread + row
        scores.append((done + low, skill / members - spread / (members * (members - 1.0))))
    if copies:
        for start, score in scores:
            for copy in range(copies):
                out[copy, start : start + score.shape[0]] = score
    else:
        for start, score in scores:
            out[start : start + score.shape[0]] = score


def scored(first, members, observed, before=(), copies=0):
    count, length, cells = members.shape
    done = sum(score.shape[0] for score in before)
    shape = (done + length, cells)
    if copies:
        shape = (copies, *shape)
    vmem = pl.BlockSpec(memory_space=pltpu.VMEM)
    return pl.pallas_call(
        functools.partial(score_kernel, first, copies),
        out_shape=jax.ShapeDtypeStruct(shape, jnp.float32),
        in_specs=[vmem] * (2 + len(before)),
        out_specs=vmem,
        cost_estimate=pl.CostEstimate(
            flops=3 * count * count * length * cells // 2, bytes_accessed=4 * count * length * cells, transcendentals=0
        ),
        compiler_params=pltpu.CompilerParams(vmem_limit_bytes=16 * 1024 * 1024),
    )(members, observed, *before)


def swapped(value):
    count = lax.axis_size("dom")
    return lax.ppermute(value, "dom", [(source, source ^ 1) for source in range(count)])


def passed_on(value, cross):
    count = lax.axis_size("dom")
    pairs = []
    for source in range(count):
        side = 1 - 2 * (source % 2)
        target = source + side * (3 if cross else 2)
        if 0 <= target < count:
            pairs.append((source, target))
    return lax.ppermute(value, "dom", pairs)


def on_device(ensemble, observed, tile_weight, tile_block, tile_target, tile_count):
    groups = ensemble.shape[0]
    tiles = (ensemble, tile_weight, tile_block, tile_target, tile_count)
    far = remap(FAR, 3, 1, CHUNKS, *tiles)
    near = remap(NEAR, 6, 3, CHUNKS, *tiles)
    ahead = []
    for keep, give in far:
        from_core = swapped(give)
        same = from_core[0] + keep[0]
        ahead.append(passed_on(jnp.stack([same, from_core[1]]), False))
    scores = []
    first = 0
    for index, (keep, give) in enumerate(near):
        from_core = swapped(give)
        same = keep[0] + from_core[0] + ahead[index][0]
        cross = keep[1] + from_core[1] + ahead[index][1]
        here = keep[2] + from_core[2]
        summed = here + passed_on(same, False) + passed_on(cross, True)
        length = CHUNKS[index]
        regrouped = lax.all_to_all(summed, "mem", split_axis=0, concat_axis=0, tiled=True)
        regrouped = regrouped.reshape(8 * groups, length, 128)
        if index + 1 < len(CHUNKS):
            scores.append(scored(first, regrouped, observed))
        else:
            copies = scored(first, regrouped, observed, scores, lax.axis_size("mem"))
        first += length
    pieces = lax.all_to_all(copies, "mem", split_axis=0, concat_axis=0, tiled=True)
    return jnp.moveaxis(pieces, 0, 1).reshape(observed.shape)


def solution(mesh):
    return jax.shard_map(
        on_device,
        mesh=mesh,
        in_specs=(
            P("mem", None, "dom"),
            P(None, "dom"),
            P("dom", None, None),
            P("dom"),
            P("dom"),
            P("dom"),
        ),
        out_specs=P(None, "dom"),
        check_vma=False,
    )
```

```python
import functools

import jax
import jax.numpy as jnp
from jax import lax
from jax.experimental import pallas as pl
from jax.experimental.pallas import tpu as pltpu
from jax.sharding import PartitionSpec as P


CHUNKS = (16, 16)

FAR = {4: 0, -3: 1, -4: 2}
NEAR = {2: 0, 3: 1, 0: 2, -1: 3, -2: 4, 1: 5}
UNROLL = 4


def coded(table):
    return sum(table.get(u, 7) << (3 * (u + 4)) for u in range(-4, 5))


def remap_kernel(codes, parts, split, chunks, block_hbm, target_hbm, count_hbm, ens_hbm, weight_hbm, *rest):
    outs, (acc, ens, weights, blocks, targets, count, slots, sems) = rest[:-8], rest[-8:]
    groups, levels, _ = ens.shape
    total = targets.shape[0]
    owned = 8
    small = [
        pltpu.make_async_copy(source, target, sems.at[index])
        for index, (source, target) in enumerate(((target_hbm, targets), (count_hbm, count), (block_hbm, blocks)))
    ]
    large = [pltpu.make_async_copy(ens_hbm.at[group], ens.at[group], sems.at[3 + group]) for group in range(groups)]
    pieces = 4
    span = total // pieces
    for piece in range(pieces):
        part = pl.ds(piece * span, span)
        large.append(pltpu.make_async_copy(weight_hbm.at[part], weights.at[part], sems.at[3 + groups + piece]))
    for copy in small + large:
        copy.start()
    device = lax.axis_index("dom")
    side = 1 - 2 * lax.rem(device, 2)
    dump = parts * owned

    def cleared(tile, carry):
        acc[tile] = jnp.zeros(acc.shape[1:], jnp.float32)
        return carry

    lax.fori_loop(0, dump, cleared, 0)
    for copy in small:
        copy.wait()
    live = count[0]

    def listed(slot, found):
        target = targets[slot]
        u = side * ((target >> 3) - device)
        code = (codes >> (3 * (u + 4))) & 7
        slots[found] = slot * 256 + code * owned + (target & 7)
        return found + jnp.where((code < 7) & (slot < live), 1, 0)

    found = lax.fori_loop(0, total, listed, jnp.int32(0), unroll=8)
    for extra in range(UNROLL):
        slots[found + extra] = dump
    for copy in large:
        copy.wait()

    def added(step, carry):
        results = []
        for offset in range(UNROLL):
            entry = slots[step * UNROLL + offset]
            slot = entry >> 8
            first = pl.multiple_of(blocks[slot] * 128, 128)
            picked = ens[:, :, pl.ds(first, 128)].reshape(groups * levels, 128)
            results.append(
                (entry & 255, jnp.dot(picked, weights[slot], preferred_element_type=jnp.float32))
            )
        for tile, result in results:
            acc[tile] += result
        return carry

    lax.fori_loop(0, (found + UNROLL - 1) // UNROLL, added, 0)

    def stored(tile, carry):
        start = 0
        for index, length in enumerate(chunks):
            for low, high, out in ((0, split, outs[2 * index]), (split, parts, outs[2 * index + 1])):
                for part in range(low, high):
                    for group in range(groups):
                        out[part - low, tile, group] = acc[part * owned + tile, pl.ds(group * levels + start, length)]
            start += length
        return carry

    lax.fori_loop(0, owned, stored, 0)


def remap(table, parts, split, chunks, limit, ensemble, tile_weight, tile_block, tile_target, tile_count):
    groups, levels, _ = ensemble.shape
    slots = tile_block.shape[0]
    shapes = []
    for length in chunks:
        for count in (split, parts - split):
            shapes.append(jax.ShapeDtypeStruct((count, 8, groups, length, 128), jnp.float32))
    outs = pl.pallas_call(
        functools.partial(remap_kernel, coded(table), parts, split, chunks),
        out_shape=shapes,
        in_specs=[pl.BlockSpec(memory_space=pltpu.HBM)] * 5,
        out_specs=[pl.BlockSpec(memory_space=pltpu.VMEM)] * len(shapes),
        scratch_shapes=[
            pltpu.VMEM((parts * 8 + 1, groups * levels, 128), jnp.float32),
            pltpu.VMEM(ensemble.shape, ensemble.dtype),
            pltpu.VMEM(tile_weight.shape, tile_weight.dtype),
            pltpu.SMEM((slots,), jnp.int32),
            pltpu.SMEM((slots,), jnp.int32),
            pltpu.SMEM((1,), jnp.int32),
            pltpu.SMEM((slots + UNROLL,), jnp.int32),
            pltpu.SemaphoreType.DMA((3 + groups + 4,)),
        ],
        cost_estimate=pl.CostEstimate(
            flops=2 * slots * groups * levels * 128 * 128, bytes_accessed=12_000_000, transcendentals=0
        ),
        compiler_params=pltpu.CompilerParams(vmem_limit_bytes=limit * 1024 * 1024),
    )(tile_block, tile_target, tile_count, ensemble, tile_weight)
    return [outs[2 * index : 2 * index + 2] for index in range(len(chunks))]


def score_kernel(first, copies, members_ref, observed_ref, *rest):
    before, out = rest[:-1], rest[-1]
    members, length, cells = members_ref.shape
    column = pl.multiple_of(lax.axis_index("mem") * cells, cells)
    done = 0
    scores = []
    for ref in before:
        scores.append((done, ref[...]))
        done += ref.shape[0]
    for low in range(0, length, 8):
        observed = observed_ref[pl.ds(first + low, 8), pl.ds(column, cells)]
        skill = jnp.zeros((8, cells), jnp.float32)
        spread = jnp.zeros((8, cells), jnp.float32)
        values = [members_ref[member, pl.ds(low, 8)] for member in range(members)]
        for left in range(members):
            skill = skill + jnp.abs(values[left] - observed)
            row = None
            for right in range(left + 1, members):
                gap = jnp.abs(values[left] - values[right])
                row = gap if row is None else row + gap
            if row is not None:
                spread = spread + row
        scores.append((done + low, skill / members - spread / (members * (members - 1.0))))
    if copies:
        for start, score in scores:
            for copy in range(copies):
                out[copy, start : start + score.shape[0]] = score
    else:
        for start, score in scores:
            out[start : start + score.shape[0]] = score


def scored(first, members, observed, before=(), copies=0):
    count, length, cells = members.shape
    done = sum(score.shape[0] for score in before)
    shape = (done + length, cells)
    if copies:
        shape = (copies, *shape)
    vmem = pl.BlockSpec(memory_space=pltpu.VMEM)
    return pl.pallas_call(
        functools.partial(score_kernel, first, copies),
        out_shape=jax.ShapeDtypeStruct(shape, jnp.float32),
        in_specs=[vmem] * (2 + len(before)),
        out_specs=vmem,
        cost_estimate=pl.CostEstimate(
            flops=3 * count * count * length * cells // 2, bytes_accessed=4 * count * length * cells, transcendentals=0
        ),
        compiler_params=pltpu.CompilerParams(vmem_limit_bytes=16 * 1024 * 1024),
    )(members, observed, *before)


def swapped(value):
    count = lax.axis_size("dom")
    return lax.ppermute(value, "dom", [(source, source ^ 1) for source in range(count)])


def passed_on(value, cross):
    count = lax.axis_size("dom")
    pairs = []
    for source in range(count):
        side = 1 - 2 * (source % 2)
        target = source + side * (3 if cross else 2)
        if 0 <= target < count:
            pairs.append((source, target))
    return lax.ppermute(value, "dom", pairs)


def on_device(ensemble, observed, tile_weight, tile_block, tile_target, tile_count):
    groups, levels, _ = ensemble.shape
    tiles = (ensemble, tile_weight, tile_block, tile_target, tile_count)
    far = remap(FAR, 3, 1, CHUNKS, 61, *tiles)
    ahead = []
    for keep, give in far:
        from_core = swapped(give)
        message = lax.dynamic_update_slice_in_dim(from_core, from_core[:1] + keep, 0, 0)
        ahead.append(passed_on(message, False))
    ((keep, give),) = remap(NEAR, 6, 3, (levels,), 18, *tiles)
    from_core = swapped(give)
    hops = []
    first = 0
    before = None
    for index, length in enumerate(CHUNKS):
        part = slice(first, first + length)
        farther = ahead[index]
        if index:
            farther, before = lax.optimization_barrier((farther, before))
        same = keep[0, :, :, part] + from_core[0, :, :, part] + farther[0]
        cross = keep[1, :, :, part] + from_core[1, :, :, part] + farther[1]
        before = same
        same = passed_on(same, False)
        cross = passed_on(cross, True)
        hops.append((same, cross))
        first += length
    scores = []
    first = 0
    for index, length in enumerate(CHUNKS):
        part = slice(first, first + length)
        arrived = hops[index]
        if index:
            arrived, before = lax.optimization_barrier((arrived, summed))
        summed = keep[2, :, :, part] + from_core[2, :, :, part] + arrived[0] + arrived[1]
        regrouped = lax.all_to_all(summed, "mem", split_axis=0, concat_axis=0, tiled=True)
        regrouped = regrouped.reshape(8 * groups, length, 128)
        if index + 1 < len(CHUNKS):
            scores.append(scored(first, regrouped, observed))
        else:
            copies = scored(first, regrouped, observed, scores, lax.axis_size("mem"))
        first += length
    pieces = lax.all_to_all(copies, "mem", split_axis=0, concat_axis=0, tiled=True)
    return jnp.moveaxis(pieces, 0, 1).reshape(observed.shape)


def solution(mesh):
    return jax.shard_map(
        on_device,
        mesh=mesh,
        in_specs=(
            P("mem", None, "dom"),
            P(None, "dom"),
            P("dom", None, None),
            P("dom"),
            P("dom"),
            P("dom"),
        ),
        out_specs=P(None, "dom"),
        check_vma=False,
    )
```

```python
import functools

import jax
import jax.numpy as jnp
from jax import lax
from jax.experimental import pallas as pl
from jax.experimental.pallas import tpu as pltpu
from jax.sharding import PartitionSpec as P


CHUNKS = (16, 16)

FAR = {4: 0, -3: 1, -4: 2}
NEAR = {2: 0, 3: 1, 0: 2, -1: 3, -2: 4, 1: 5}
UNROLL = 4


def coded(table):
    return sum(table.get(u, 7) << (3 * (u + 4)) for u in range(-4, 5))


def remap_kernel(codes, parts, load, block_hbm, target_hbm, count_hbm, ens_in, weight_in, *rest):
    outs, (acc, blocks, targets, count, slots, sems) = rest[:-6], rest[-6:]
    ens, weights = ens_in, weight_in
    if load:
        *outs, ens, weights = outs
    groups, levels, _ = ens_in.shape
    total = targets.shape[0]
    owned = 8
    small = [
        pltpu.make_async_copy(source, target, sems.at[index])
        for index, (source, target) in enumerate(((target_hbm, targets), (count_hbm, count), (block_hbm, blocks)))
    ]
    large = []
    if load:
        pieces = 4
        span = total // pieces
        for group in range(groups):
            large.append(pltpu.make_async_copy(ens_in.at[group], ens.at[group], sems.at[3 + group]))
        for piece in range(pieces):
            part = pl.ds(piece * span, span)
            large.append(pltpu.make_async_copy(weight_in.at[part], weights.at[part], sems.at[3 + groups + piece]))
    for copy in small + large:
        copy.start()
    device = lax.axis_index("dom")
    side = 1 - 2 * lax.rem(device, 2)
    dump = parts * owned

    def cleared(tile, carry):
        acc[tile] = jnp.zeros(acc.shape[1:], jnp.float32)
        return carry

    lax.fori_loop(0, dump, cleared, 0)
    for copy in small:
        copy.wait()
    live = count[0]

    def listed(slot, found):
        target = targets[slot]
        u = side * ((target >> 3) - device)
        code = (codes >> (3 * (u + 4))) & 7
        slots[found] = slot * 256 + code * owned + (target & 7)
        return found + jnp.where((code < 7) & (slot < live), 1, 0)

    found = lax.fori_loop(0, total, listed, jnp.int32(0), unroll=8)
    for extra in range(UNROLL):
        slots[found + extra] = dump
    for copy in large:
        copy.wait()

    def added(step, carry):
        results = []
        for offset in range(UNROLL):
            entry = slots[step * UNROLL + offset]
            slot = entry >> 8
            first = pl.multiple_of(blocks[slot] * 128, 128)
            picked = ens[:, :, pl.ds(first, 128)].reshape(groups * levels, 128)
            results.append(
                (entry & 255, jnp.dot(picked, weights[slot], preferred_element_type=jnp.float32))
            )
        for tile, result in results:
            acc[tile] += result
        return carry

    lax.fori_loop(0, (found + UNROLL - 1) // UNROLL, added, 0)

    def stored(tile, carry):
        part = 0
        for out in outs:
            for place in range(out.shape[0]):
                for group in range(groups):
                    out[place, tile, group] = acc[part * owned + tile, pl.ds(group * levels, levels)]
                part += 1
        return carry

    lax.fori_loop(0, owned, stored, 0)


def remap(table, splits, load, ensemble, tile_weight, tile_block, tile_target, tile_count):
    groups, levels, _ = ensemble.shape
    slots = tile_block.shape[0]
    parts = sum(splits)
    shapes = [jax.ShapeDtypeStruct((count, 8, groups, levels, 128), jnp.float32) for count in splits]
    if load:
        shapes += [jax.ShapeDtypeStruct(value.shape, value.dtype) for value in (ensemble, tile_weight)]
    hbm = pl.BlockSpec(memory_space=pltpu.HBM)
    vmem = pl.BlockSpec(memory_space=pltpu.VMEM)
    return pl.pallas_call(
        functools.partial(remap_kernel, coded(table), parts, load),
        out_shape=shapes,
        in_specs=[hbm] * 3 + [hbm if load else vmem] * 2,
        out_specs=[vmem] * len(shapes),
        scratch_shapes=[
            pltpu.VMEM((parts * 8 + 1, groups * levels, 128), jnp.float32),
            pltpu.SMEM((slots,), jnp.int32),
            pltpu.SMEM((slots,), jnp.int32),
            pltpu.SMEM((1,), jnp.int32),
            pltpu.SMEM((slots + UNROLL,), jnp.int32),
            pltpu.SemaphoreType.DMA((3 + groups + 4,)),
        ],
        cost_estimate=pl.CostEstimate(
            flops=2 * slots * groups * levels * 128 * 128, bytes_accessed=12_000_000, transcendentals=0
        ),
        compiler_params=pltpu.CompilerParams(vmem_limit_bytes=18 * 1024 * 1024),
    )(tile_block, tile_target, tile_count, ensemble, tile_weight)


def score_kernel(first, copies, members_ref, observed_ref, *rest):
    before, out = rest[:-1], rest[-1]
    members, length, cells = members_ref.shape
    column = pl.multiple_of(lax.axis_index("mem") * cells, cells)
    done = 0
    scores = []
    for ref in before:
        scores.append((done, ref[...]))
        done += ref.shape[0]
    for low in range(0, length, 8):
        observed = observed_ref[pl.ds(first + low, 8), pl.ds(column, cells)]
        skill = jnp.zeros((8, cells), jnp.float32)
        spread = jnp.zeros((8, cells), jnp.float32)
        values = [members_ref[member, pl.ds(low, 8)] for member in range(members)]
        for left in range(members):
            skill = skill + jnp.abs(values[left] - observed)
            row = None
            for right in range(left + 1, members):
                gap = jnp.abs(values[left] - values[right])
                row = gap if row is None else row + gap
            if row is not None:
                spread = spread + row
        scores.append((done + low, skill / members - spread / (members * (members - 1.0))))
    if copies:
        for start, score in scores:
            for copy in range(copies):
                out[copy, start : start + score.shape[0]] = score
    else:
        for start, score in scores:
            out[start : start + score.shape[0]] = score


def scored(first, members, observed, before=(), copies=0):
    count, length, cells = members.shape
    done = sum(score.shape[0] for score in before)
    shape = (done + length, cells)
    if copies:
        shape = (copies, *shape)
    vmem = pl.BlockSpec(memory_space=pltpu.VMEM)
    return pl.pallas_call(
        functools.partial(score_kernel, first, copies),
        out_shape=jax.ShapeDtypeStruct(shape, jnp.float32),
        in_specs=[vmem] * (2 + len(before)),
        out_specs=vmem,
        cost_estimate=pl.CostEstimate(
            flops=3 * count * count * length * cells // 2, bytes_accessed=4 * count * length * cells, transcendentals=0
        ),
        compiler_params=pltpu.CompilerParams(vmem_limit_bytes=16 * 1024 * 1024),
    )(members, observed, *before)


def swapped(value):
    count = lax.axis_size("dom")
    return lax.ppermute(value, "dom", [(source, source ^ 1) for source in range(count)])


def passed_on(value, cross):
    count = lax.axis_size("dom")
    pairs = []
    for source in range(count):
        side = 1 - 2 * (source % 2)
        target = source + side * (3 if cross else 2)
        if 0 <= target < count:
            pairs.append((source, target))
    return lax.ppermute(value, "dom", pairs)


def on_device(ensemble, observed, tile_weight, tile_block, tile_target, tile_count):
    groups, _, _ = ensemble.shape
    tiles = (ensemble, tile_weight, tile_block, tile_target, tile_count)
    tiles = tuple(pltpu.with_memory_space_constraint(value, pltpu.HBM) for value in tiles[:4]) + tiles[4:]
    keep, give, *held = remap(FAR, (1, 2), True, *tiles)
    from_core = swapped(give)
    ahead = []
    first = 0
    for length in CHUNKS:
        part = slice(first, first + length)
        value = jnp.concatenate([from_core[:1, :, :, part] + keep[:, :, :, part], from_core[1:, :, :, part]])
        ahead.append(passed_on(value, False))
        first += length
    keep, own, give = remap(NEAR, (2, 1, 3), False, *held, *tiles[2:])
    from_core = swapped(give)
    here = own[0] + from_core[2]
    hops = []
    first = 0
    before = None
    for index, length in enumerate(CHUNKS):
        part = slice(first, first + length)
        farther = ahead[index]
        if index:
            farther, before = lax.optimization_barrier((farther, before))
        same = keep[0, :, :, part] + from_core[0, :, :, part] + farther[0]
        cross = keep[1, :, :, part] + from_core[1, :, :, part] + farther[1]
        before = same
        same = passed_on(same, False)
        cross = passed_on(cross, True)
        hops.append((same, cross))
        first += length
    scores = []
    first = 0
    for index, length in enumerate(CHUNKS):
        part = slice(first, first + length)
        arrived = hops[index]
        if index:
            arrived, before = lax.optimization_barrier((arrived, summed))
        summed = here[:, :, part] + arrived[0] + arrived[1]
        regrouped = lax.all_to_all(summed, "mem", split_axis=0, concat_axis=0, tiled=True)
        regrouped = regrouped.reshape(8 * groups, length, 128)
        if index + 1 < len(CHUNKS):
            scores.append(scored(first, regrouped, observed))
        else:
            copies = scored(first, regrouped, observed, scores, lax.axis_size("mem"))
        first += length
    pieces = lax.all_to_all(copies, "mem", split_axis=0, concat_axis=0, tiled=True)
    return jnp.moveaxis(pieces, 0, 1).reshape(observed.shape)


def solution(mesh):
    return jax.shard_map(
        on_device,
        mesh=mesh,
        in_specs=(
            P("mem", None, "dom"),
            P(None, "dom"),
            P("dom", None, None),
            P("dom"),
            P("dom"),
            P("dom"),
        ),
        out_specs=P(None, "dom"),
        check_vma=False,
    )
```

```python
import functools

import jax
import jax.numpy as jnp
from jax import lax
from jax.experimental import pallas as pl
from jax.experimental.pallas import tpu as pltpu
from jax.sharding import PartitionSpec as P


CHUNKS = (8, 24)

FAR = {4: 0, -3: 1, -4: 2}
NEAR = {2: 0, 3: 1, 0: 2, -1: 3, -2: 4, 1: 5}
UNROLL = 4


def coded(table):
    return sum(table.get(u, 7) << (3 * (u + 4)) for u in range(-4, 5))


def remap_kernel(codes, parts, load, block_hbm, target_hbm, count_hbm, ens_in, weight_in, *rest):
    outs, (acc, blocks, targets, count, slots, sems) = rest[:-6], rest[-6:]
    ens, weights = ens_in, weight_in
    if load:
        *outs, ens, weights = outs
    groups, levels, _ = ens_in.shape
    total = targets.shape[0]
    owned = 8
    small = [
        pltpu.make_async_copy(source, target, sems.at[index])
        for index, (source, target) in enumerate(((target_hbm, targets), (count_hbm, count), (block_hbm, blocks)))
    ]
    large = []
    if load:
        pieces = 4
        span = total // pieces
        for group in range(groups):
            large.append(pltpu.make_async_copy(ens_in.at[group], ens.at[group], sems.at[3 + group]))
        for piece in range(pieces):
            part = pl.ds(piece * span, span)
            large.append(pltpu.make_async_copy(weight_in.at[part], weights.at[part], sems.at[3 + groups + piece]))
    for copy in small + large:
        copy.start()
    device = lax.axis_index("dom")
    side = 1 - 2 * lax.rem(device, 2)
    dump = parts * owned

    def cleared(tile, carry):
        acc[tile] = jnp.zeros(acc.shape[1:], jnp.float32)
        return carry

    lax.fori_loop(0, dump, cleared, 0)
    for copy in small:
        copy.wait()
    live = count[0]

    def listed(slot, found):
        target = targets[slot]
        u = side * ((target >> 3) - device)
        code = (codes >> (3 * (u + 4))) & 7
        slots[found] = slot * 256 + code * owned + (target & 7)
        return found + jnp.where((code < 7) & (slot < live), 1, 0)

    found = lax.fori_loop(0, total, listed, jnp.int32(0), unroll=8)
    for extra in range(UNROLL):
        slots[found + extra] = dump
    for copy in large:
        copy.wait()

    def added(step, carry):
        results = []
        for offset in range(UNROLL):
            entry = slots[step * UNROLL + offset]
            slot = entry >> 8
            first = pl.multiple_of(blocks[slot] * 128, 128)
            picked = ens[:, :, pl.ds(first, 128)].reshape(groups * levels, 128)
            results.append(
                (entry & 255, jnp.dot(picked, weights[slot], preferred_element_type=jnp.float32))
            )
        for tile, result in results:
            acc[tile] += result
        return carry

    lax.fori_loop(0, (found + UNROLL - 1) // UNROLL, added, 0)

    def stored(tile, carry):
        part = 0
        for out in outs:
            for place in range(out.shape[0]):
                for group in range(groups):
                    out[place, tile, group] = acc[part * owned + tile, pl.ds(group * levels, levels)]
                part += 1
        return carry

    lax.fori_loop(0, owned, stored, 0)


def remap(table, splits, load, ensemble, tile_weight, tile_block, tile_target, tile_count):
    groups, levels, _ = ensemble.shape
    slots = tile_block.shape[0]
    parts = sum(splits)
    shapes = [jax.ShapeDtypeStruct((count, 8, groups, levels, 128), jnp.float32) for count in splits]
    if load:
        shapes += [jax.ShapeDtypeStruct(value.shape, value.dtype) for value in (ensemble, tile_weight)]
    hbm = pl.BlockSpec(memory_space=pltpu.HBM)
    vmem = pl.BlockSpec(memory_space=pltpu.VMEM)
    return pl.pallas_call(
        functools.partial(remap_kernel, coded(table), parts, load),
        out_shape=shapes,
        in_specs=[hbm] * 3 + [hbm if load else vmem] * 2,
        out_specs=[vmem] * len(shapes),
        scratch_shapes=[
            pltpu.VMEM((parts * 8 + 1, groups * levels, 128), jnp.float32),
            pltpu.SMEM((slots,), jnp.int32),
            pltpu.SMEM((slots,), jnp.int32),
            pltpu.SMEM((1,), jnp.int32),
            pltpu.SMEM((slots + UNROLL,), jnp.int32),
            pltpu.SemaphoreType.DMA((3 + groups + 4,)),
        ],
        cost_estimate=pl.CostEstimate(
            flops=2 * slots * groups * levels * 128 * 128, bytes_accessed=12_000_000, transcendentals=0
        ),
        compiler_params=pltpu.CompilerParams(vmem_limit_bytes=16 * 1024 * 1024),
    )(tile_block, tile_target, tile_count, ensemble, tile_weight)


def score_kernel(first, copies, members_ref, observed_ref, *rest):
    before, out = rest[:-1], rest[-1]
    members, length, cells = members_ref.shape
    column = pl.multiple_of(lax.axis_index("mem") * cells, cells)
    done = 0
    scores = []
    for ref in before:
        scores.append((done, ref[...]))
        done += ref.shape[0]
    for low in range(0, length, 8):
        observed = observed_ref[pl.ds(first + low, 8), pl.ds(column, cells)]
        skill = jnp.zeros((8, cells), jnp.float32)
        spread = jnp.zeros((8, cells), jnp.float32)
        values = [members_ref[member, pl.ds(low, 8)] for member in range(members)]
        for left in range(members):
            skill = skill + jnp.abs(values[left] - observed)
            row = None
            for right in range(left + 1, members):
                gap = jnp.abs(values[left] - values[right])
                row = gap if row is None else row + gap
            if row is not None:
                spread = spread + row
        scores.append((done + low, skill / members - spread / (members * (members - 1.0))))
    if copies:
        for start, score in scores:
            for copy in range(copies):
                out[copy, start : start + score.shape[0]] = score
    else:
        for start, score in scores:
            out[start : start + score.shape[0]] = score


def scored(first, members, observed, before=(), copies=0):
    count, length, cells = members.shape
    done = sum(score.shape[0] for score in before)
    shape = (done + length, cells)
    if copies:
        shape = (copies, *shape)
    vmem = pl.BlockSpec(memory_space=pltpu.VMEM)
    return pl.pallas_call(
        functools.partial(score_kernel, first, copies),
        out_shape=jax.ShapeDtypeStruct(shape, jnp.float32),
        in_specs=[vmem] * (2 + len(before)),
        out_specs=vmem,
        cost_estimate=pl.CostEstimate(
            flops=3 * count * count * length * cells // 2, bytes_accessed=4 * count * length * cells, transcendentals=0
        ),
        compiler_params=pltpu.CompilerParams(vmem_limit_bytes=8 * 1024 * 1024),
    )(members, observed, *before)


def swapped(value):
    count = lax.axis_size("dom")
    return lax.ppermute(value, "dom", [(source, source ^ 1) for source in range(count)])


def passed_on(value, cross):
    count = lax.axis_size("dom")
    pairs = []
    for source in range(count):
        side = 1 - 2 * (source % 2)
        target = source + side * (3 if cross else 2)
        if 0 <= target < count:
            pairs.append((source, target))
    return lax.ppermute(value, "dom", pairs)


def on_device(ensemble, observed, tile_weight, tile_block, tile_target, tile_count):
    groups, levels, _ = ensemble.shape
    tiles = (ensemble, tile_weight, tile_block, tile_target, tile_count)
    tiles = tuple(pltpu.with_memory_space_constraint(value, pltpu.HBM) for value in tiles[:4]) + tiles[4:]
    keep, give, *held = remap(FAR, (1, 2), True, *tiles)
    from_core = swapped(give)
    ahead = []
    first = 0
    for length in CHUNKS:
        part = slice(first, first + length)
        value = jnp.concatenate([from_core[:1, :, :, part] + keep[:, :, :, part], from_core[1:, :, :, part]])
        ahead.append(passed_on(value, False))
        first += length
    keep, own, give = remap(NEAR, (2, 1, 3), False, *held, *tiles[2:])
    from_core = swapped(give)
    here, nearby = lax.optimization_barrier((own[0] + from_core[2], keep + from_core[:2]))

    def led(index, first):
        part = slice(first, first + CHUNKS[index])
        return [nearby[way, :, :, part] + ahead[index][way] for way in (0, 1)]

    turned = CHUNKS[0]
    both = led(0, 0)
    both = jnp.stack([*both, here[:, :, :turned]], axis=1)
    mixed = lax.all_to_all(both, "mem", split_axis=0, concat_axis=0, tiled=True)
    before = both
    first = turned
    starts = []
    for index in range(1, len(CHUNKS)):
        ahead[index], before = lax.optimization_barrier((ahead[index], before))
        before = led(index, first)
        starts.append(before)
        first += CHUNKS[index]
    first = turned
    arrived = []
    for index, (same, cross) in enumerate(starts, 1):
        same = passed_on(same, False)
        cross = passed_on(cross, True)
        arrived.append((same, cross, here[:, :, first : first + CHUNKS[index]]))
        first += CHUNKS[index]
    same, cross, rest = (mixed[:, way] for way in range(3))
    same = passed_on(same, False)
    cross = passed_on(cross, True)
    summed = [one + two + three for one, two, three in arrived]
    summed = summed[0] if len(summed) == 1 else jnp.concatenate(summed, axis=2)
    regrouped = lax.all_to_all(summed, "mem", split_axis=0, concat_axis=0, tiled=True)
    regrouped = regrouped.reshape(8 * groups, levels - turned, 128)
    near_first = (rest + same + cross).reshape(8 * groups, turned, 128)
    score = scored(0, near_first, observed)
    copies = scored(turned, regrouped, observed, (score,), lax.axis_size("mem"))
    pieces = lax.all_to_all(copies, "mem", split_axis=0, concat_axis=0, tiled=True)
    return jnp.moveaxis(pieces, 0, 1).reshape(observed.shape)


def solution(mesh):
    return jax.shard_map(
        on_device,
        mesh=mesh,
        in_specs=(
            P("mem", None, "dom"),
            P(None, "dom"),
            P("dom", None, None),
            P("dom"),
            P("dom"),
            P("dom"),
        ),
        out_specs=P(None, "dom"),
        check_vma=False,
    )
```

```python
import functools

import jax
import jax.numpy as jnp
from jax import lax
from jax.experimental import pallas as pl
from jax.experimental.pallas import tpu as pltpu
from jax.sharding import PartitionSpec as P


CHUNKS = (8, 24)

FAR = {4: 0, -3: 1, -4: 2}
NEAR = {2: 0, 3: 1, 0: 2, -1: 3, -2: 4, 1: 5}
UNROLL = 4


def coded(table):
    return sum(table.get(u, 7) << (3 * (u + 4)) for u in range(-4, 5))


def remap_kernel(codes, parts, load, block_hbm, target_hbm, count_hbm, ens_in, weight_in, *rest):
    outs, (acc, blocks, targets, count, slots, sems) = rest[:-6], rest[-6:]
    ens, weights = ens_in, weight_in
    if load:
        *outs, ens, weights = outs
    groups, levels, _ = ens_in.shape
    total = targets.shape[0]
    owned = 8
    small = [
        pltpu.make_async_copy(source, target, sems.at[index])
        for index, (source, target) in enumerate(((target_hbm, targets), (count_hbm, count), (block_hbm, blocks)))
    ]
    large = []
    if load:
        pieces = 4
        span = total // pieces
        for group in range(groups):
            large.append(pltpu.make_async_copy(ens_in.at[group], ens.at[group], sems.at[3 + group]))
        for piece in range(pieces):
            part = pl.ds(piece * span, span)
            large.append(pltpu.make_async_copy(weight_in.at[part], weights.at[part], sems.at[3 + groups + piece]))
    for copy in small + large:
        copy.start()
    device = lax.axis_index("dom")
    side = 1 - 2 * lax.rem(device, 2)
    dump = parts * owned

    def cleared(tile, carry):
        acc[tile] = jnp.zeros(acc.shape[1:], jnp.float32)
        return carry

    lax.fori_loop(0, dump, cleared, 0)
    for copy in small:
        copy.wait()
    live = count[0]

    def listed(slot, found):
        target = targets[slot]
        u = side * ((target >> 3) - device)
        code = (codes >> (3 * (u + 4))) & 7
        slots[found] = slot * 256 + code * owned + (target & 7)
        return found + jnp.where((code < 7) & (slot < live), 1, 0)

    pieces = 4
    span = total // pieces
    found = jnp.int32(0)
    ends = []
    for piece in range(pieces):
        found = lax.fori_loop(piece * span, (piece + 1) * span, listed, found, unroll=8)
        ends.append(found)
    for extra in range(UNROLL):
        slots[found + extra] = dump

    def added(step, carry):
        results = []
        for offset in range(UNROLL):
            entry = slots[step * UNROLL + offset]
            slot = entry >> 8
            first = pl.multiple_of(blocks[slot] * 128, 128)
            picked = ens[:, :, pl.ds(first, 128)].reshape(groups * levels, 128)
            results.append(
                (entry & 255, jnp.dot(picked, weights[slot], preferred_element_type=jnp.float32))
            )
        for tile, result in results:
            acc[tile] += result
        return carry

    steps = [end // UNROLL for end in ends[:-1]] + [(found + UNROLL - 1) // UNROLL]
    if load:
        for copy in large[:groups]:
            copy.wait()
        begin = 0
        for copy, step in zip(large[groups:], steps):
            copy.wait()
            lax.fori_loop(begin, step, added, 0)
            begin = step
    else:
        lax.fori_loop(0, steps[-1], added, 0)

    def stored(tile, carry):
        part = 0
        for out in outs:
            for place in range(out.shape[0]):
                for group in range(groups):
                    out[place, tile, group] = acc[part * owned + tile, pl.ds(group * levels, levels)]
                part += 1
        return carry

    lax.fori_loop(0, owned, stored, 0)


def remap(table, splits, load, ensemble, tile_weight, tile_block, tile_target, tile_count):
    groups, levels, _ = ensemble.shape
    slots = tile_block.shape[0]
    parts = sum(splits)
    shapes = [jax.ShapeDtypeStruct((count, 8, groups, levels, 128), jnp.float32) for count in splits]
    if load:
        shapes += [jax.ShapeDtypeStruct(value.shape, value.dtype) for value in (ensemble, tile_weight)]
    hbm = pl.BlockSpec(memory_space=pltpu.HBM)
    vmem = pl.BlockSpec(memory_space=pltpu.VMEM)
    return pl.pallas_call(
        functools.partial(remap_kernel, coded(table), parts, load),
        out_shape=shapes,
        in_specs=[hbm] * 3 + [hbm if load else vmem] * 2,
        out_specs=[vmem] * len(shapes),
        scratch_shapes=[
            pltpu.VMEM((parts * 8 + 1, groups * levels, 128), jnp.float32),
            pltpu.SMEM((slots,), jnp.int32),
            pltpu.SMEM((slots,), jnp.int32),
            pltpu.SMEM((1,), jnp.int32),
            pltpu.SMEM((slots + UNROLL,), jnp.int32),
            pltpu.SemaphoreType.DMA((3 + groups + 4,)),
        ],
        cost_estimate=pl.CostEstimate(
            flops=2 * slots * groups * levels * 128 * 128, bytes_accessed=12_000_000, transcendentals=0
        ),
        compiler_params=pltpu.CompilerParams(vmem_limit_bytes=18 * 1024 * 1024),
    )(tile_block, tile_target, tile_count, ensemble, tile_weight)


def comparators(count):
    found = []
    half = 1
    while half < count:
        step = half
        while step >= 1:
            for start in range(step % half, count - step, 2 * step):
                for place in range(start, min(start + step, count - step)):
                    if place // (2 * half) == (place + step) // (2 * half):
                        found.append((place, place + step))
            step //= 2
        half *= 2
    return found


def score_kernel(first, copies, members_ref, observed_ref, *rest):
    before, out = rest[:-1], rest[-1]
    members, length, cells = members_ref.shape
    column = pl.multiple_of(lax.axis_index("mem") * cells, cells)
    done = 0
    scores = []
    for ref in before:
        scores.append((done, ref[...]))
        done += ref.shape[0]
    for low in range(0, length, 8):
        observed = observed_ref[pl.ds(first + low, 8), pl.ds(column, cells)]
        skill = jnp.zeros((8, cells), jnp.float32)
        spread = jnp.zeros((8, cells), jnp.float32)
        values = [members_ref[member, pl.ds(low, 8)] for member in range(members)]
        for value in values:
            skill = skill + jnp.abs(value - observed)
        for under, over in comparators(members):
            values[under], values[over] = (
                jnp.minimum(values[under], values[over]),
                jnp.maximum(values[under], values[over]),
            )
        for below in range(members - 1):
            pairs = float((below + 1) * (members - 1 - below))
            spread = spread + pairs * (values[below + 1] - values[below])
        scores.append((done + low, skill / members - spread / (members * (members - 1.0))))
    if copies:
        for start, score in scores:
            for copy in range(copies):
                out[copy, start : start + score.shape[0]] = score
    else:
        for start, score in scores:
            out[start : start + score.shape[0]] = score


def scored(first, members, observed, before=(), copies=0):
    count, length, cells = members.shape
    done = sum(score.shape[0] for score in before)
    shape = (done + length, cells)
    if copies:
        shape = (copies, *shape)
    vmem = pl.BlockSpec(memory_space=pltpu.VMEM)
    return pl.pallas_call(
        functools.partial(score_kernel, first, copies),
        out_shape=jax.ShapeDtypeStruct(shape, jnp.float32),
        in_specs=[vmem] * (2 + len(before)),
        out_specs=vmem,
        cost_estimate=pl.CostEstimate(
            flops=3 * count * count * length * cells // 2, bytes_accessed=4 * count * length * cells, transcendentals=0
        ),
        compiler_params=pltpu.CompilerParams(vmem_limit_bytes=16 * 1024 * 1024),
    )(members, observed, *before)


def swapped(value):
    count = lax.axis_size("dom")
    return lax.ppermute(value, "dom", [(source, source ^ 1) for source in range(count)])


def passed_on(value, cross):
    count = lax.axis_size("dom")
    pairs = []
    for source in range(count):
        side = 1 - 2 * (source % 2)
        target = source + side * (3 if cross else 2)
        if 0 <= target < count:
            pairs.append((source, target))
    return lax.ppermute(value, "dom", pairs)


def on_device(ensemble, observed, tile_weight, tile_block, tile_target, tile_count):
    groups, _, _ = ensemble.shape
    tiles = (ensemble, tile_weight, tile_block, tile_target, tile_count)
    tiles = tuple(pltpu.with_memory_space_constraint(value, pltpu.HBM) for value in tiles[:4]) + tiles[4:]
    keep, give, *held = remap(FAR, (1, 2), True, *tiles)
    from_core = swapped(give)
    ahead = []
    first = 0
    for length in CHUNKS:
        part = slice(first, first + length)
        value = jnp.concatenate([from_core[:1, :, :, part] + keep[:, :, :, part], from_core[1:, :, :, part]])
        ahead.append(passed_on(value, False))
        first += length
    keep, own, give = remap(NEAR, (2, 1, 3), False, *held, *tiles[2:])
    from_core = swapped(give)
    here = own[0] + from_core[2]
    hops = []
    first = 0
    before = None
    for index, length in enumerate(CHUNKS):
        part = slice(first, first + length)
        farther = ahead[index]
        if index:
            farther, before = lax.optimization_barrier((farther, before))
        same = keep[0, :, :, part] + from_core[0, :, :, part] + farther[0]
        cross = keep[1, :, :, part] + from_core[1, :, :, part] + farther[1]
        before = same
        same = passed_on(same, False)
        cross = passed_on(cross, True)
        hops.append((same, cross))
        first += length
    scores = []
    first = 0
    for index, length in enumerate(CHUNKS):
        part = slice(first, first + length)
        arrived = hops[index]
        if index:
            arrived, before = lax.optimization_barrier((arrived, summed))
        summed = here[:, :, part] + arrived[0] + arrived[1]
        regrouped = lax.all_to_all(summed, "mem", split_axis=0, concat_axis=0, tiled=True)
        regrouped = regrouped.reshape(8 * groups, length, 128)
        if index + 1 < len(CHUNKS):
            scores.append(scored(first, regrouped, observed))
        else:
            copies = scored(first, regrouped, observed, scores, lax.axis_size("mem"))
        first += length
    pieces = lax.all_to_all(copies, "mem", split_axis=0, concat_axis=0, tiled=True)
    return jnp.moveaxis(pieces, 0, 1).reshape(observed.shape)


def solution(mesh):
    return jax.shard_map(
        on_device,
        mesh=mesh,
        in_specs=(
            P("mem", None, "dom"),
            P(None, "dom"),
            P("dom", None, None),
            P("dom"),
            P("dom"),
            P("dom"),
        ),
        out_specs=P(None, "dom"),
        check_vma=False,
    )
```

```python
import functools

import jax
import jax.numpy as jnp
from jax import lax
from jax.experimental import pallas as pl
from jax.experimental.pallas import tpu as pltpu
from jax.sharding import PartitionSpec as P


CHUNKS = (16, 16)
MIXES = ((0, 1),)

FAR = {4: 0, -3: 1, -4: 2}
NEAR = {2: 0, 3: 1, 0: 2, -1: 3, -2: 4, 1: 5}
UNROLL = 4


def coded(table):
    return sum(table.get(u, 7) << (3 * (u + 4)) for u in range(-4, 5))


def remap_kernel(codes, parts, load, block_hbm, target_hbm, count_hbm, ens_in, weight_in, *rest):
    outs, (acc, blocks, targets, count, slots, sems) = rest[:-6], rest[-6:]
    ens, weights = ens_in, weight_in
    if load:
        *outs, ens, weights = outs
    groups, levels, _ = ens_in.shape
    total = targets.shape[0]
    owned = 8
    small = [
        pltpu.make_async_copy(source, target, sems.at[index])
        for index, (source, target) in enumerate(((target_hbm, targets), (count_hbm, count), (block_hbm, blocks)))
    ]
    large = []
    if load:
        pieces = 4
        span = total // pieces
        for group in range(groups):
            large.append(pltpu.make_async_copy(ens_in.at[group], ens.at[group], sems.at[3 + group]))
        for piece in range(pieces):
            part = pl.ds(piece * span, span)
            large.append(pltpu.make_async_copy(weight_in.at[part], weights.at[part], sems.at[3 + groups + piece]))
    for copy in small + large:
        copy.start()
    device = lax.axis_index("dom")
    side = 1 - 2 * lax.rem(device, 2)
    dump = parts * owned

    def cleared(tile, carry):
        acc[tile] = jnp.zeros(acc.shape[1:], jnp.float32)
        return carry

    lax.fori_loop(0, dump, cleared, 0)
    for copy in small:
        copy.wait()
    live = count[0]

    def listed(slot, found):
        target = targets[slot]
        u = side * ((target >> 3) - device)
        code = (codes >> (3 * (u + 4))) & 7
        slots[found] = slot * 256 + code * owned + (target & 7)
        return found + jnp.where((code < 7) & (slot < live), 1, 0)

    pieces = 4
    span = total // pieces
    found = jnp.int32(0)
    ends = []
    for piece in range(pieces):
        found = lax.fori_loop(piece * span, (piece + 1) * span, listed, found, unroll=8)
        ends.append(found)
    for extra in range(UNROLL):
        slots[found + extra] = dump

    def added(step, carry):
        results = []
        for offset in range(UNROLL):
            entry = slots[step * UNROLL + offset]
            slot = entry >> 8
            first = pl.multiple_of(blocks[slot] * 128, 128)
            picked = ens[:, :, pl.ds(first, 128)].reshape(groups * levels, 128)
            results.append(
                (entry & 255, jnp.dot(picked, weights[slot], preferred_element_type=jnp.float32))
            )
        for tile, result in results:
            acc[tile] += result
        return carry

    steps = [end // UNROLL for end in ends[:-1]] + [(found + UNROLL - 1) // UNROLL]
    if load:
        for copy in large[:groups]:
            copy.wait()
        begin = 0
        for copy, step in zip(large[groups:], steps):
            copy.wait()
            lax.fori_loop(begin, step, added, 0)
            begin = step
    else:
        lax.fori_loop(0, steps[-1], added, 0)

    def stored(tile, carry):
        part = 0
        for out in outs:
            for place in range(out.shape[0]):
                for group in range(groups):
                    out[place, tile, group] = acc[part * owned + tile, pl.ds(group * levels, levels)]
                part += 1
        return carry

    lax.fori_loop(0, owned, stored, 0)


def remap(table, splits, load, ensemble, tile_weight, tile_block, tile_target, tile_count):
    groups, levels, _ = ensemble.shape
    slots = tile_block.shape[0]
    parts = sum(splits)
    shapes = [jax.ShapeDtypeStruct((count, 8, groups, levels, 128), jnp.float32) for count in splits]
    if load:
        shapes += [jax.ShapeDtypeStruct(value.shape, value.dtype) for value in (ensemble, tile_weight)]
    hbm = pl.BlockSpec(memory_space=pltpu.HBM)
    vmem = pl.BlockSpec(memory_space=pltpu.VMEM)
    return pl.pallas_call(
        functools.partial(remap_kernel, coded(table), parts, load),
        out_shape=shapes,
        in_specs=[hbm] * 3 + [hbm if load else vmem] * 2,
        out_specs=[vmem] * len(shapes),
        scratch_shapes=[
            pltpu.VMEM((parts * 8 + 1, groups * levels, 128), jnp.float32),
            pltpu.SMEM((slots,), jnp.int32),
            pltpu.SMEM((slots,), jnp.int32),
            pltpu.SMEM((1,), jnp.int32),
            pltpu.SMEM((slots + UNROLL,), jnp.int32),
            pltpu.SemaphoreType.DMA((3 + groups + 4,)),
        ],
        cost_estimate=pl.CostEstimate(
            flops=2 * slots * groups * levels * 128 * 128, bytes_accessed=12_000_000, transcendentals=0
        ),
        compiler_params=pltpu.CompilerParams(vmem_limit_bytes=18 * 1024 * 1024),
    )(tile_block, tile_target, tile_count, ensemble, tile_weight)


def comparators(count):
    found = []
    half = 1
    while half < count:
        step = half
        while step >= 1:
            for start in range(step % half, count - step, 2 * step):
                for place in range(start, min(start + step, count - step)):
                    if place // (2 * half) == (place + step) // (2 * half):
                        found.append((place, place + step))
            step //= 2
        half *= 2
    return found


def score_kernel(first, copies, members_ref, observed_ref, *rest):
    before, out = rest[:-1], rest[-1]
    members, length, cells = members_ref.shape
    column = pl.multiple_of(lax.axis_index("mem") * cells, cells)
    done = 0
    scores = []
    for ref in before:
        scores.append((done, ref[...]))
        done += ref.shape[0]
    for low in range(0, length, 8):
        observed = observed_ref[pl.ds(first + low, 8), pl.ds(column, cells)]
        skill = jnp.zeros((8, cells), jnp.float32)
        spread = jnp.zeros((8, cells), jnp.float32)
        values = [members_ref[member, pl.ds(low, 8)] for member in range(members)]
        for value in values:
            skill = skill + jnp.abs(value - observed)
        for under, over in comparators(members):
            values[under], values[over] = (
                jnp.minimum(values[under], values[over]),
                jnp.maximum(values[under], values[over]),
            )
        for below in range(members - 1):
            pairs = float((below + 1) * (members - 1 - below))
            spread = spread + pairs * (values[below + 1] - values[below])
        scores.append((done + low, skill / members - spread / (members * (members - 1.0))))
    if copies:
        for start, score in scores:
            for copy in range(copies):
                out[copy, start : start + score.shape[0]] = score
    else:
        for start, score in scores:
            out[start : start + score.shape[0]] = score


def scored(first, members, observed, before=(), copies=0):
    count, length, cells = members.shape
    done = sum(score.shape[0] for score in before)
    shape = (done + length, cells)
    if copies:
        shape = (copies, *shape)
    vmem = pl.BlockSpec(memory_space=pltpu.VMEM)
    return pl.pallas_call(
        functools.partial(score_kernel, first, copies),
        out_shape=jax.ShapeDtypeStruct(shape, jnp.float32),
        in_specs=[vmem] * (2 + len(before)),
        out_specs=vmem,
        cost_estimate=pl.CostEstimate(
            flops=3 * count * count * length * cells // 2, bytes_accessed=4 * count * length * cells, transcendentals=0
        ),
        compiler_params=pltpu.CompilerParams(vmem_limit_bytes=16 * 1024 * 1024),
    )(members, observed, *before)


def swapped(value):
    count = lax.axis_size("dom")
    return lax.ppermute(value, "dom", [(source, source ^ 1) for source in range(count)])


def passed_on(value, cross):
    count = lax.axis_size("dom")
    pairs = []
    for source in range(count):
        side = 1 - 2 * (source % 2)
        target = source + side * (3 if cross else 2)
        if 0 <= target < count:
            pairs.append((source, target))
    return lax.ppermute(value, "dom", pairs)


def on_device(ensemble, observed, tile_weight, tile_block, tile_target, tile_count):
    groups, _, _ = ensemble.shape
    tiles = (ensemble, tile_weight, tile_block, tile_target, tile_count)
    tiles = tuple(pltpu.with_memory_space_constraint(value, pltpu.HBM) for value in tiles[:4]) + tiles[4:]
    keep, give, *held = remap(FAR, (1, 2), True, *tiles)
    from_core = swapped(give)
    ahead = []
    first = 0
    for length in CHUNKS:
        part = slice(first, first + length)
        value = jnp.concatenate([from_core[:1, :, :, part] + keep[:, :, :, part], from_core[1:, :, :, part]])
        ahead.append(passed_on(value, False))
        first += length
    keep, own, give = remap(NEAR, (2, 1, 3), False, *held, *tiles[2:])
    from_core = swapped(give)
    here = own[0] + from_core[2]
    hops = []
    first = 0
    before = None
    for index, length in enumerate(CHUNKS):
        part = slice(first, first + length)
        farther = ahead[index]
        if index:
            farther, before = lax.optimization_barrier((farther, before))
        same = keep[0, :, :, part] + from_core[0, :, :, part] + farther[0]
        cross = keep[1, :, :, part] + from_core[1, :, :, part] + farther[1]
        before = same
        same = passed_on(same, False)
        cross = passed_on(cross, True)
        hops.append((same, cross))
        first += length
    scores = []
    first = 0
    summed = None
    for mix, members in enumerate(MIXES):
        begin = first
        totals = []
        for index in members:
            part = slice(first, first + CHUNKS[index])
            arrived = hops[index]
            if summed is not None:
                arrived, before = lax.optimization_barrier((arrived, summed))
            summed = here[:, :, part] + arrived[0] + arrived[1]
            totals.append(summed)
            first += CHUNKS[index]
        if len(totals) > 1:
            totals = [jnp.concatenate(totals, axis=2)]
        regrouped = lax.all_to_all(totals[0], "mem", split_axis=0, concat_axis=0, tiled=True)
        regrouped = regrouped.reshape(8 * groups, first - begin, 128)
        if mix + 1 < len(MIXES):
            scores.append(scored(begin, regrouped, observed))
        else:
            copies = scored(begin, regrouped, observed, scores, lax.axis_size("mem"))
    pieces = lax.all_to_all(copies, "mem", split_axis=0, concat_axis=0, tiled=True)
    return jnp.moveaxis(pieces, 0, 1).reshape(observed.shape)


def solution(mesh):
    return jax.shard_map(
        on_device,
        mesh=mesh,
        in_specs=(
            P("mem", None, "dom"),
            P(None, "dom"),
            P("dom", None, None),
            P("dom"),
            P("dom"),
            P("dom"),
        ),
        out_specs=P(None, "dom"),
        check_vma=False,
    )
```

```python
import functools

import jax
import jax.numpy as jnp
from jax import lax
from jax.experimental import pallas as pl
from jax.experimental.pallas import tpu as pltpu
from jax.sharding import PartitionSpec as P


CHUNKS = (16, 16)
MIXES = ((0, 1),)

FAR = {4: 0, -3: 2, -4: 3}
NEAR = {2: 0, 3: 1, 0: 2, -1: 3, -2: 4, 1: 5}
UNROLL = 4


def coded(table):
    return sum(table.get(u, 7) << (3 * (u + 4)) for u in range(-4, 5))


def remap_kernel(codes, parts, load, block_hbm, target_hbm, count_hbm, ens_in, weight_in, *rest):
    outs, (acc, blocks, targets, count, slots, sems) = rest[:-6], rest[-6:]
    ens, weights = ens_in, weight_in
    if load:
        *outs, ens, weights = outs
    groups, levels, _ = ens_in.shape
    total = targets.shape[0]
    owned = 8
    small = [
        pltpu.make_async_copy(source, target, sems.at[index])
        for index, (source, target) in enumerate(((target_hbm, targets), (count_hbm, count), (block_hbm, blocks)))
    ]
    large = []
    if load:
        pieces = 4
        span = total // pieces
        for group in range(groups):
            large.append(pltpu.make_async_copy(ens_in.at[group], ens.at[group], sems.at[3 + group]))
        for piece in range(pieces):
            part = pl.ds(piece * span, span)
            large.append(pltpu.make_async_copy(weight_in.at[part], weights.at[part], sems.at[3 + groups + piece]))
    for copy in small + large:
        copy.start()
    device = lax.axis_index("dom")
    side = 1 - 2 * lax.rem(device, 2)
    dump = parts * owned

    def cleared(tile, carry):
        acc[tile] = jnp.zeros(acc.shape[1:], jnp.float32)
        return carry

    lax.fori_loop(0, dump, cleared, 0)
    for copy in small:
        copy.wait()
    live = count[0]

    def listed(slot, found):
        target = targets[slot]
        u = side * ((target >> 3) - device)
        code = (codes >> (3 * (u + 4))) & 7
        slots[found] = slot * 256 + code * owned + (target & 7)
        return found + jnp.where((code < 7) & (slot < live), 1, 0)

    pieces = 4
    span = total // pieces
    found = jnp.int32(0)
    ends = []
    for piece in range(pieces):
        found = lax.fori_loop(piece * span, (piece + 1) * span, listed, found, unroll=8)
        ends.append(found)
    for extra in range(UNROLL):
        slots[found + extra] = dump

    def added(step, carry):
        results = []
        for offset in range(UNROLL):
            entry = slots[step * UNROLL + offset]
            slot = entry >> 8
            first = pl.multiple_of(blocks[slot] * 128, 128)
            picked = ens[:, :, pl.ds(first, 128)].reshape(groups * levels, 128)
            results.append(
                (entry & 255, jnp.dot(picked, weights[slot], preferred_element_type=jnp.float32))
            )
        for tile, result in results:
            acc[tile] += result
        return carry

    steps = [end // UNROLL for end in ends[:-1]] + [(found + UNROLL - 1) // UNROLL]
    if load:
        for copy in large[:groups]:
            copy.wait()
        begin = 0
        for copy, step in zip(large[groups:], steps):
            copy.wait()
            lax.fori_loop(begin, step, added, 0)
            begin = step
    else:
        lax.fori_loop(0, steps[-1], added, 0)

    def stored(tile, carry):
        part = 0
        for out in outs:
            for place in range(out.shape[0]):
                for group in range(groups):
                    out[place, tile, group] = acc[part * owned + tile, pl.ds(group * levels, levels)]
                part += 1
        return carry

    lax.fori_loop(0, owned, stored, 0)


def remap(table, splits, load, ensemble, tile_weight, tile_block, tile_target, tile_count):
    groups, levels, _ = ensemble.shape
    slots = tile_block.shape[0]
    parts = sum(splits)
    shapes = [jax.ShapeDtypeStruct((count, 8, groups, levels, 128), jnp.float32) for count in splits]
    if load:
        shapes += [jax.ShapeDtypeStruct(value.shape, value.dtype) for value in (ensemble, tile_weight)]
    hbm = pl.BlockSpec(memory_space=pltpu.HBM)
    vmem = pl.BlockSpec(memory_space=pltpu.VMEM)
    return pl.pallas_call(
        functools.partial(remap_kernel, coded(table), parts, load),
        out_shape=shapes,
        in_specs=[hbm] * 3 + [hbm if load else vmem] * 2,
        out_specs=[vmem] * len(shapes),
        scratch_shapes=[
            pltpu.VMEM((parts * 8 + 1, groups * levels, 128), jnp.float32),
            pltpu.SMEM((slots,), jnp.int32),
            pltpu.SMEM((slots,), jnp.int32),
            pltpu.SMEM((1,), jnp.int32),
            pltpu.SMEM((slots + UNROLL,), jnp.int32),
            pltpu.SemaphoreType.DMA((3 + groups + 4,)),
        ],
        cost_estimate=pl.CostEstimate(
            flops=2 * slots * groups * levels * 128 * 128, bytes_accessed=12_000_000, transcendentals=0
        ),
        compiler_params=pltpu.CompilerParams(vmem_limit_bytes=18 * 1024 * 1024),
    )(tile_block, tile_target, tile_count, ensemble, tile_weight)


def comparators(count):
    found = []
    half = 1
    while half < count:
        step = half
        while step >= 1:
            for start in range(step % half, count - step, 2 * step):
                for place in range(start, min(start + step, count - step)):
                    if place // (2 * half) == (place + step) // (2 * half):
                        found.append((place, place + step))
            step //= 2
        half *= 2
    return found


def score_kernel(first, copies, members_ref, observed_ref, *rest):
    before, out = rest[:-1], rest[-1]
    members, length, cells = members_ref.shape
    column = pl.multiple_of(lax.axis_index("mem") * cells, cells)
    done = 0
    scores = []
    for ref in before:
        scores.append((done, ref[...]))
        done += ref.shape[0]
    for low in range(0, length, 8):
        observed = observed_ref[pl.ds(first + low, 8), pl.ds(column, cells)]
        skill = jnp.zeros((8, cells), jnp.float32)
        spread = jnp.zeros((8, cells), jnp.float32)
        values = [members_ref[member, pl.ds(low, 8)] for member in range(members)]
        for value in values:
            skill = skill + jnp.abs(value - observed)
        for under, over in comparators(members):
            values[under], values[over] = (
                jnp.minimum(values[under], values[over]),
                jnp.maximum(values[under], values[over]),
            )
        for below in range(members - 1):
            pairs = float((below + 1) * (members - 1 - below))
            spread = spread + pairs * (values[below + 1] - values[below])
        scores.append((done + low, skill / members - spread / (members * (members - 1.0))))
    if copies:
        for start, score in scores:
            for copy in range(copies):
                out[copy, start : start + score.shape[0]] = score
    else:
        for start, score in scores:
            out[start : start + score.shape[0]] = score


def scored(first, members, observed, before=(), copies=0):
    count, length, cells = members.shape
    done = sum(score.shape[0] for score in before)
    shape = (done + length, cells)
    if copies:
        shape = (copies, *shape)
    vmem = pl.BlockSpec(memory_space=pltpu.VMEM)
    return pl.pallas_call(
        functools.partial(score_kernel, first, copies),
        out_shape=jax.ShapeDtypeStruct(shape, jnp.float32),
        in_specs=[vmem] * (2 + len(before)),
        out_specs=vmem,
        cost_estimate=pl.CostEstimate(
            flops=3 * count * count * length * cells // 2, bytes_accessed=4 * count * length * cells, transcendentals=0
        ),
        compiler_params=pltpu.CompilerParams(vmem_limit_bytes=16 * 1024 * 1024),
    )(members, observed, *before)


def swapped(value):
    count = lax.axis_size("dom")
    return lax.ppermute(value, "dom", [(source, source ^ 1) for source in range(count)])


def passed_on(value, cross):
    count = lax.axis_size("dom")
    pairs = []
    for source in range(count):
        side = 1 - 2 * (source % 2)
        target = source + side * (3 if cross else 2)
        if 0 <= target < count:
            pairs.append((source, target))
    return lax.ppermute(value, "dom", pairs)


def on_device(ensemble, observed, tile_weight, tile_block, tile_target, tile_count):
    groups, _, _ = ensemble.shape
    tiles = (ensemble, tile_weight, tile_block, tile_target, tile_count)
    tiles = tuple(pltpu.with_memory_space_constraint(value, pltpu.HBM) for value in tiles[:4]) + tiles[4:]
    keep, give, *held = remap(FAR, (2, 2), True, *tiles)
    from_core = swapped(give)
    ahead = []
    first = 0
    for length in CHUNKS:
        part = slice(first, first + length)
        value = from_core[:, :, :, part] + keep[:, :, :, part]
        ahead.append(passed_on(value, False))
        first += length
    keep, own, give = remap(NEAR, (2, 1, 3), False, *held, *tiles[2:])
    from_core = swapped(give)
    here = own[0] + from_core[2]
    hops = []
    first = 0
    before = None
    for index, length in enumerate(CHUNKS):
        part = slice(first, first + length)
        farther = ahead[index]
        if index:
            farther, before = lax.optimization_barrier((farther, before))
        same = keep[0, :, :, part] + from_core[0, :, :, part] + farther[0]
        cross = keep[1, :, :, part] + from_core[1, :, :, part] + farther[1]
        before = same
        same = passed_on(same, False)
        cross = passed_on(cross, True)
        hops.append((same, cross))
        first += length
    scores = []
    first = 0
    summed = None
    for mix, members in enumerate(MIXES):
        begin = first
        totals = []
        for index in members:
            part = slice(first, first + CHUNKS[index])
            arrived = hops[index]
            if summed is not None:
                arrived, before = lax.optimization_barrier((arrived, summed))
            summed = here[:, :, part] + arrived[0] + arrived[1]
            totals.append(summed)
            first += CHUNKS[index]
        if len(totals) > 1:
            totals = [jnp.concatenate(totals, axis=2)]
        regrouped = lax.all_to_all(totals[0], "mem", split_axis=0, concat_axis=0, tiled=True)
        regrouped = regrouped.reshape(8 * groups, first - begin, 128)
        if mix + 1 < len(MIXES):
            scores.append(scored(begin, regrouped, observed))
        else:
            copies = scored(begin, regrouped, observed, scores, lax.axis_size("mem"))
    pieces = lax.all_to_all(copies, "mem", split_axis=0, concat_axis=0, tiled=True)
    return jnp.moveaxis(pieces, 0, 1).reshape(observed.shape)


def solution(mesh):
    return jax.shard_map(
        on_device,
        mesh=mesh,
        in_specs=(
            P("mem", None, "dom"),
            P(None, "dom"),
            P("dom", None, None),
            P("dom"),
            P("dom"),
            P("dom"),
        ),
        out_specs=P(None, "dom"),
        check_vma=False,
    )
```
